256 devices in a mesh: ctx: 128 (over x, z, y), tp: 2 (over core).
Axes of the slice: x: 4, y: 4, z: 8, core: 2. Of those that a mesh axis runs over, the one named last changes fastest.
Arguments:
- queries: bfloat16 [24576, 32, 128], P('ctx', 'tp'), may hold values from -6 to 6
- key_vectors: bfloat16 [24576, 4, 128], P('ctx', 'tp'), may hold values from -6 to 6
- value_matrix: bfloat16 [24576, 4, 128], P('ctx', 'tp'), may hold values from -6 to 6
- grad_out: bfloat16 [24576, 32, 128], P('ctx', 'tp'), may hold values from -6 to 6
- doc_lengths: int32 [64], replicated, may hold values from 1 to 1345, 24576 in all
Outputs:
- grad_queries: bfloat16 [24576, 32, 128], P('ctx', 'tp')
- grad_keys: bfloat16 [24576, 4, 128], P('ctx', 'tp')
- grad_values: bfloat16 [24576, 4, 128], P('ctx', 'tp')
The draws below stay inside these ranges and needn't reach their ends.
Inputs may be any that keep to these rules, and one draw needn't show every extreme that they name: `doc_lengths`: 64 document lengths that sum to 24576; the longest is exactly 1345.
All inputs are finite; a program needn't handle non-finite values.
Results may differ from the reference program's by a relative error of at most 0.0079.
Values may be sent and summed in bfloat16 or wider, within the bound.
A program may use at most 64 MiB of HBM per device.

```python
import math
import jax
import jax.numpy as jnp
import numpy as np
from jax import lax

QUERY_HEADS = 32
VALUE_HEADS = 4
HEAD_SIZE = 128
TOK_DEV = 192
WIN = 8
SEQUENCE_TOKENS = 24576
MAXDOC = 1345
NDOCS = 64
N_CTX = 128


def draw_queries(key, part):
    array_shape = (SEQUENCE_TOKENS, QUERY_HEADS, HEAD_SIZE)
    noise = jnp.clip(jax.random.normal(jax.random.fold_in(key, 11), array_shape, jnp.float32), -4.0, 4.0)
    return noise.astype(jnp.bfloat16)


def draw_key_vectors(key, part):
    array_shape = (SEQUENCE_TOKENS, VALUE_HEADS, HEAD_SIZE)
    noise = jnp.clip(jax.random.normal(jax.random.fold_in(key, 12), array_shape, jnp.float32), -4.0, 4.0)
    return noise.astype(jnp.bfloat16)


def level_of(stream_key, shape, pieces, least, high):
    factor_of = 1.0
    for axis_at, parts in pieces:
        draws = jax.random.uniform(jax.random.fold_in(jax.random.fold_in(stream_key, 6), axis_at), (parts,), jnp.float32, least / len(pieces), high / len(pieces))
        factor_of = factor_of * jnp.repeat(jnp.exp(draws), shape[axis_at] // parts).reshape((-1,) + (1,) * (len(shape) - 1 - axis_at))
    return factor_of


def length_profile(count, total, limit, slope):
    weights = [(1 << 20) // math.isqrt(grade ** slope) + 1 for grade in range(2, count + 1)]
    surplus, counts = total - limit - (count - 1), [1] * (count - 1)
    while surplus > 0:
        free = [i for i in range(count - 1) if counts[i] < limit]
        whole, left = sum([weights[i] for i in free]), surplus
        for i in free:
            addition = min(limit - counts[i], max(1, left * weights[i] // whole), surplus)
            counts[i] = counts[i] + addition
            surplus = surplus - addition
    return np.array([limit] + counts)


def ragged_sizes(key, number_of, total, most, skew):
    if number_of == 2:
        one = jax.random.randint(key, (), max(1, total - most), min(most, total - 1) + 1)
        return jnp.stack([one, total - one])
    tallies = jnp.asarray(length_profile(number_of, total, most, skew), jnp.int32)
    pairs = (number_of - 1) // 2
    source_of, receiver = tallies[1:1 + 2 * pairs:2], tallies[2:2 + 2 * pairs:2]
    slack = jnp.minimum(source_of - 1, most - receiver)
    moved = jax.random.randint(jax.random.fold_in(key, 1), (pairs,), 0, 1 << 20) % (slack + 1)
    tallies = tallies.at[1:1 + 2 * pairs:2].set(source_of - moved).at[2:2 + 2 * pairs:2].set(receiver + moved)
    return tallies[jax.random.permutation(jax.random.fold_in(key, 2), number_of)]


def gaussian(key, dims, width, limit, split=(), held_as=jnp.bfloat16):
    drawn = jax.random.normal(key, dims, jnp.float32) * width
    if len(split) > 0:
        drawn = level_of(key, dims, split, -0.22, 0.18) * drawn
    return jnp.clip(drawn, min=-limit, max=limit).astype(held_as)


def setup_inputs(seed: int = 0) -> dict:
    arg_keys = jax.random.split(jax.random.key(seed), 6)
    return {
        "queries": draw_queries(jax.random.fold_in(arg_keys[5], 71), 0),
        "key_vectors": draw_key_vectors(jax.random.fold_in(arg_keys[5], 71), 0),
        "value_matrix": gaussian(arg_keys[2], (SEQUENCE_TOKENS, VALUE_HEADS, HEAD_SIZE), 1.0, 6.0, ((0, 128), (1, 2))),
        "grad_out": gaussian(arg_keys[3], (SEQUENCE_TOKENS, QUERY_HEADS, HEAD_SIZE), 1.0, 6.0, ((0, 128), (1, 2))),
        "doc_lengths": ragged_sizes(arg_keys[4], NDOCS, SEQUENCE_TOKENS, MAXDOC, 2).astype(jnp.int32),
    }


neg_fill = -1.0e30


def doc_index(positions, lengths):
    doc_ends = jnp.cumsum(lengths)
    return jnp.sum((positions[:, None] >= doc_ends[None, :]).astype(jnp.int32), axis=1).astype(jnp.int32)


def reference(queries, key_vectors, value_matrix, grad_out, doc_lengths):
    stripe = TOK_DEV
    key_span = WIN * TOK_DEV
    leading_rows = key_span - stripe
    head_groups = VALUE_HEADS
    repeat_factor = QUERY_HEADS // VALUE_HEADS
    softmax_scale = HEAD_SIZE ** -0.5
    highest = lax.Precision.HIGHEST
    leading_zeros = jnp.zeros((leading_rows, VALUE_HEADS, HEAD_SIZE), jnp.float32)
    padded_keys = jnp.concatenate([leading_zeros, key_vectors.astype(jnp.float32)], axis=0)
    padded_values = jnp.concatenate([leading_zeros, value_matrix.astype(jnp.float32)], axis=0)
    query_all = queries.astype(jnp.float32).reshape(N_CTX, stripe, head_groups, repeat_factor, HEAD_SIZE)
    grad_all = grad_out.astype(jnp.float32).reshape(N_CTX, stripe, head_groups, repeat_factor, HEAD_SIZE)
    numbers = jnp.arange(N_CTX, dtype=jnp.int32)

    def one_stripe(carried, inputs):
        key_acc, value_acc = carried
        query_rows, grad_rows, number = inputs
        start = (number * stripe).astype(jnp.int32)
        key_win = lax.dynamic_slice_in_dim(padded_keys, start, key_span, 0)
        value_win = lax.dynamic_slice_in_dim(padded_values, start, key_span, 0)
        query_pos = start + jnp.arange(stripe, dtype=jnp.int32)
        key_pos = start - leading_rows + jnp.arange(key_span, dtype=jnp.int32)
        same_doc = doc_index(key_pos, doc_lengths)[None, :] == doc_index(query_pos, doc_lengths)[:, None]
        live_pairs = (key_pos[None, :] <= query_pos[:, None]) & (key_pos[None, :] >= 0) & same_doc
        raw_scores = jnp.einsum("qgrd,kgd->grqk", query_rows, key_win, precision=highest) * softmax_scale
        logits = jnp.where(live_pairs, raw_scores, neg_fill)
        row_max = jnp.max(logits, axis=-1, keepdims=True)
        row_sum = jnp.sum(jnp.where(live_pairs, jnp.exp(logits - row_max), 0.0), axis=-1, keepdims=True)
        log_total = row_max + jnp.log(row_sum)
        probs = jnp.where(live_pairs, jnp.exp(logits - log_total), 0.0)
        grad_probs = jnp.einsum("qgrd,kgd->grqk", grad_rows, value_win, precision=highest)
        row_dots = jnp.sum(probs * grad_probs, axis=-1, keepdims=True)
        grad_scores = lax.optimization_barrier((probs * (grad_probs - row_dots)).astype(jnp.bfloat16)).astype(jnp.float32)
        probs_low = lax.optimization_barrier(probs.astype(jnp.bfloat16)).astype(jnp.float32)
        query_grad = jnp.einsum("grqk,kgd->qgrd", grad_scores, key_win, precision=highest) * softmax_scale
        key_grad = jnp.einsum("grqk,qgrd->kgd", grad_scores, query_rows, precision=highest) * softmax_scale
        value_grad = jnp.einsum("grqk,qgrd->kgd", probs_low, grad_rows, precision=highest)
        key_acc = lax.dynamic_update_slice_in_dim(key_acc, lax.dynamic_slice_in_dim(key_acc, start, key_span, 0) + key_grad, start, 0)
        value_acc = lax.dynamic_update_slice_in_dim(value_acc, lax.dynamic_slice_in_dim(value_acc, start, key_span, 0) + value_grad, start, 0)
        return (key_acc, value_acc), query_grad.reshape(stripe, QUERY_HEADS, HEAD_SIZE).astype(jnp.bfloat16)

    initial_accumulator = jnp.zeros((leading_rows + SEQUENCE_TOKENS, VALUE_HEADS, HEAD_SIZE), jnp.float32)
    (key_acc, value_acc), query_parts = lax.scan(one_stripe, (initial_accumulator, initial_accumulator), (query_all, grad_all, numbers))
    grad_queries = query_parts.reshape(SEQUENCE_TOKENS, QUERY_HEADS, HEAD_SIZE)
    grad_keys = key_acc[leading_rows:].astype(jnp.bfloat16)
    grad_values = value_acc[leading_rows:].astype(jnp.bfloat16)
    return (grad_queries, grad_keys, grad_values)
```

```python
import functools

import jax
import jax.numpy as jnp
from jax import lax
from jax.experimental import pallas as pl
from jax.experimental.pallas import tpu as pltpu
from jax.sharding import PartitionSpec as P

RING = 4
SLOTS = 8
FAN = 8
DIM = 128
QTILE = 256
GROUPS = 2
LOG2E = 1.4426950408889634
DEAD = -1e30


def program_order():
    a = lambda s, c: ("A", s, c)
    f = lambda s, g: ("F", s, g)
    b = lambda s, g: ("B", s, g)
    r = lambda s, g: ("R", s, g)
    return [
        f(0, 0), f(0, 1),
        a(4, 0), a(1, 0), a(4, 1), a(1, 1), f(4, 0),
        a(4, 2), a(1, 2), a(3, 0), f(1, 0),
        a(4, 3), a(1, 3), a(3, 1), a(5, 0), f(3, 0),
        f(4, 1), a(5, 1), a(3, 2), f(5, 0),
        a(3, 3), a(5, 2), a(7, 0), f(1, 1),
        a(5, 3), a(7, 1), a(2, 0), a(2, 1), f(7, 0),
        f(2, 0), a(7, 2), f(3, 1), a(7, 3), f(5, 1),
        a(6, 0), a(6, 1), f(6, 0), ("S", 0, 0), b(6, 0), r(6, 0),
        b(2, 0), r(2, 0), a(2, 2), a(2, 3), f(2, 1), f(7, 1),
        b(7, 0), b(5, 0), a(6, 2), a(6, 3), f(6, 1), ("S", 0, 1), b(6, 1), r(6, 1),
        r(7, 0), r(5, 0), b(2, 1), r(2, 1), b(3, 0), b(1, 0),
        b(7, 1), r(3, 0), r(1, 0), r(7, 1), b(5, 1), r(5, 1),
        b(4, 0), b(3, 1), b(1, 1), r(4, 0), r(3, 1), r(1, 1), b(0, 0),
        b(4, 1), r(4, 1), b(0, 1), ("Q", 0, 0), ("Q", 0, 1),
        r(0, 0), r(0, 1),
    ]


def kernel(
    tok, nctx, ndocs, q_hbm, k_hbm, v_hbm, do_hbm, len_ref, dq_hbm, dk_hbm, dv_hbm,
    qin, doin, kin, vin, wide, kv, qrow, qcol, orow, ocol, start_ref, pos_ref,
    mst, lst, dst_, prob, gprob, plow, dscore, grad, sbuf, rbuf, dqf, outk, outv, outq,
    in_sem, out_sem, fs_sem, fr_sem, rs_sem, rr_sem,
):
    me = lax.axis_index("ctx")
    y = lax.rem(me, RING)
    row = me - y
    up = row + lax.rem(y + 1, RING)
    down = row + lax.rem(y + RING - 1, RING)
    ahead = lax.rem(me + RING, nctx)
    behind = lax.rem(me + nctx - RING, nctx)
    qrows = tok * FAN
    tiles = qrows // QTILE
    scale = DIM**-0.5

    copies = [
        pltpu.make_async_copy(k_hbm, kin, in_sem.at[0]),
        pltpu.make_async_copy(v_hbm, vin, in_sem.at[1]),
        pltpu.make_async_copy(q_hbm, qin, in_sem.at[2]),
        pltpu.make_async_copy(do_hbm, doin, in_sem.at[3]),
    ]
    for copy in copies:
        copy.start()
    barrier = pltpu.get_barrier_semaphore()
    for other in (up, down, ahead, behind):
        pl.semaphore_signal(
            barrier, inc=1, device_id={"ctx": other}, device_id_type=pl.DeviceIdType.MESH
        )
    for which, source in enumerate((kin, vin)):
        copies[which].wait()
        wide[which] = source[...].astype(jnp.float32)
        for g in range(GROUPS):
            kv[g, which, 0:tok] = wide[which, pl.ds(g, tok, stride=GROUPS), :].astype(jnp.bfloat16)
    pl.semaphore_wait(barrier, 4)

    fetch = {
        1: (up, jnp.where(y < RING - 1, 0, 4)),
        2: (up, jnp.where(y < RING - 1, 1, 5)),
        3: (down, jnp.where(y > 0, 4, 0)),
        4: (ahead, 0),
        5: (ahead, 1),
        6: (down, jnp.where(y > 0, 7, 3)),
        7: (ahead, 3),
    }
    parent = {1: down, 2: down, 3: up, 4: behind, 5: behind, 6: up, 7: behind}

    def fetch_copy(slot, c):
        target, source = fetch[slot]
        g, which = c // 2, c % 2
        rows = pl.ds(pl.multiple_of(source * tok, 16), tok)
        return pltpu.make_async_remote_copy(
            src_ref=kv.at[g, which, rows],
            dst_ref=kv.at[g, which, pl.ds(slot * tok, tok)],
            send_sem=fs_sem.at[slot - 1, c],
            recv_sem=fr_sem.at[slot - 1, c],
            device_id={"ctx": target},
            device_id_type=pl.DeviceIdType.MESH,
        )

    def return_copy(slot, c):
        return pltpu.make_async_remote_copy(
            src_ref=sbuf.at[slot - 1, c],
            dst_ref=rbuf.at[slot - 1, c],
            send_sem=rs_sem.at[slot - 1, c],
            recv_sem=rr_sem.at[slot - 1, c],
            device_id={"ctx": parent[slot]},
            device_id_type=pl.DeviceIdType.MESH,
        )

    def start_if(condition, slot, c):
        if condition is None:
            fetch_copy(slot, c).start()
        else:

            @pl.when(condition)
            def _():
                fetch_copy(slot, c).start()

    for c in range(4):
        start_if(None, 4, c)
        start_if(y < RING - 1, 1, c)
        start_if(y == 0, 3, c)

    forwards = {
        1: ((5, None), (2, y < RING - 1)),
        4: ((1, y == RING - 1), (3, y > 0)),
        3: ((7, None), (6, y == 0)),
        5: ((2, y == RING - 1),),
        7: ((6, y > 0),),
        2: (),
        6: (),
    }

    def arrive(slot, c):
        fetch_copy(slot, c).wait_recv()
        for onward, condition in forwards[slot]:
            start_if(condition, onward, c)

    step = QTILE // FAN
    for which, (source, rows_ref, cols_ref) in enumerate(((qin, qrow, qcol), (doin, orow, ocol))):
        copies[2 + which].wait()

        @pl.loop(0, tok // step)
        def _(n):
            block = source[pl.ds(n * step, step)].astype(jnp.float32)
            at = pl.ds(pl.multiple_of(n * QTILE, QTILE), QTILE)
            for g in range(GROUPS):
                part = block[:, g * FAN : (g + 1) * FAN, :].reshape(QTILE, DIM)
                rows_ref[g, at, :] = part.astype(jnp.bfloat16)
                cols_ref[g, :, at] = part.T.astype(jnp.bfloat16)

    pos = me * tok + lax.shift_right_logical(lax.broadcasted_iota(jnp.int32, (1, qrows), 1), 3)

    def doc_step(n, carried):
        end, begin = carried
        end = end + len_ref[n]
        return end, jnp.where(pos >= end, end, begin)

    unused, begin = lax.fori_loop(0, ndocs, doc_step, (jnp.int32(0), jnp.zeros_like(pos)))
    start_ref[...] = begin
    pos_ref[...] = pos

    last = {0: None, 1: None}

    def first_pass(slot, g):
        rows = slice(slot * tok, (slot + 1) * tok)
        keys, values = kv[g, 0, rows], kv[g, 1, rows]
        before = last[g]
        key_pos = (me - slot) * tok + lax.broadcasted_iota(jnp.int32, (tok, QTILE), 0)
        for n in range(tiles):
            at = slice(n * QTILE, (n + 1) * QTILE)
            scores = jnp.dot(keys, qcol[g, :, at], preferred_element_type=jnp.float32)
            grads = jnp.dot(values, ocol[g, :, at], preferred_element_type=jnp.float32)
            live = key_pos >= start_ref[:, at]
            if slot == 0:
                live = live & (key_pos <= pos_ref[:, at])
            scores = jnp.where(live, scores * (scale * LOG2E), DEAD)
            top = jnp.max(scores, axis=0, keepdims=True)
            if before is not None:
                old = mst[g, before : before + 1, at]
                top = jnp.maximum(top, old)
            probs = jnp.exp2(scores - top)
            total = jnp.sum(probs, axis=0, keepdims=True)
            dots = jnp.sum(probs * grads, axis=0, keepdims=True)
            if before is not None:
                shrink = jnp.exp2(old - top)
                total = total + lst[g : g + 1, at] * shrink
                dots = dots + dst_[g : g + 1, at] * shrink
            mst[g, slot : slot + 1, at] = top
            lst[g : g + 1, at] = total
            dst_[g : g + 1, at] = dots
            prob[g, rows, at] = probs
            gprob[g, rows, at] = grads
        last[g] = slot

    def statistics(g):
        inverse = 1.0 / lst[g : g + 1, :]
        final = mst[g, last[g] : last[g] + 1, :]
        dst_[g : g + 1, :] = dst_[g : g + 1, :] * inverse
        for slot in range(SLOTS):
            mst[g, slot : slot + 1, :] = jnp.exp2(mst[g, slot : slot + 1, :] - final) * inverse

    def second_pass(slot, g):
        rows = slice(slot * tok, (slot + 1) * tok)
        key_sum, value_sum = None, None
        for n in range(tiles):
            at = slice(n * QTILE, (n + 1) * QTILE)
            probs = prob[g, rows, at] * mst[g, slot : slot + 1, at]
            scores = probs * (gprob[g, rows, at] - dst_[g : g + 1, at])
            low, scores = probs.astype(jnp.bfloat16), scores.astype(jnp.bfloat16)
            dscore[g, rows, at] = scores
            value_part = jnp.dot(low, orow[g, at, :], preferred_element_type=jnp.float32)
            key_part = jnp.dot(scores, qrow[g, at, :], preferred_element_type=jnp.float32)
            key_sum = key_part if n == 0 else key_sum + key_part
            value_sum = value_part if n == 0 else value_sum + value_part
        if slot in (2, 6):
            sbuf[slot - 1, 2 * g] = key_sum.astype(jnp.bfloat16)
            sbuf[slot - 1, 2 * g + 1] = value_sum.astype(jnp.bfloat16)
        else:
            grad[slot, 2 * g] = key_sum
            grad[slot, 2 * g + 1] = value_sum

    takes = {
        7: ((6, y > 0),),
        5: ((2, y == RING - 1),),
        3: ((7, None), (6, y == 0)),
        1: ((5, None), (2, y < RING - 1)),
        4: ((1, y == RING - 1), (3, y > 0)),
        0: ((4, None), (1, y < RING - 1), (3, y == 0)),
    }

    def take(slot, given, c):
        return_copy(given, c).wait_recv()
        grad[slot, c] = grad[slot, c] + rbuf[given - 1, c].astype(jnp.float32)

    def give_back(slot, g):
        for c in (2 * g, 2 * g + 1):
            for given, condition in takes.get(slot, ()):
                if condition is None:
                    take(slot, given, c)
                else:
                    pl.when(condition)(functools.partial(take, slot, given, c))
            if slot in takes and slot > 0:
                sbuf[slot - 1, c] = grad[slot, c].astype(jnp.bfloat16)
            if slot > 0:
                return_copy(slot, c).start()

    def query_grads(g):
        for n in range(tiles):
            at = slice(n * QTILE, (n + 1) * QTILE)
            part = lax.dot_general(
                dscore[g, :, at], kv[g, 0], (((0,), (0,)), ((), ())),
                preferred_element_type=jnp.float32,
            )
            dqf[g, at, :] = part * scale

    acts = {
        "A": arrive, "F": first_pass, "B": second_pass, "R": give_back,
        "S": lambda unused, g: statistics(g), "Q": lambda unused, g: query_grads(g),
    }
    for kind, slot, which in program_order():
        if kind == "R" and slot == 0 and which == 0:

            @pl.loop(0, tok // step)
            def _(n):
                at = pl.ds(pl.multiple_of(n * QTILE, QTILE), QTILE)
                parts = [dqf[g, at, :].reshape(step, FAN, DIM) for g in range(GROUPS)]
                outq[pl.ds(n * step, step)] = jnp.concatenate(parts, axis=1).astype(jnp.bfloat16)

            out_q = pltpu.make_async_copy(outq, dq_hbm, out_sem.at[2])
            out_q.start()
        acts[kind](slot, which)

    for g in range(GROUPS):
        wide[0, pl.ds(g, tok, stride=GROUPS), :] = grad[0, 2 * g] * scale
        wide[1, pl.ds(g, tok, stride=GROUPS), :] = grad[0, 2 * g + 1]
    outk[...] = wide[0].astype(jnp.bfloat16)
    outv[...] = wide[1].astype(jnp.bfloat16)
    out_k = pltpu.make_async_copy(outk, dk_hbm, out_sem.at[0])
    out_v = pltpu.make_async_copy(outv, dv_hbm, out_sem.at[1])
    out_k.start()
    out_v.start()
    for slot in range(1, SLOTS):
        for c in range(4):
            fetch_copy(slot, c).wait_send()
            return_copy(slot, c).wait_send()
    out_q.wait()
    out_k.wait()
    out_v.wait()


def local(nctx, queries, key_vectors, value_matrix, grad_out, doc_lengths):
    tok, heads, dim = queries.shape
    qrows = tok * FAN
    bf, f32 = jnp.bfloat16, jnp.float32
    anywhere = pl.BlockSpec(memory_space=pl.ANY)
    dq, dk, dv = pl.pallas_call(
        functools.partial(kernel, tok, nctx, doc_lengths.shape[0]),
        out_shape=(
            jax.ShapeDtypeStruct((tok, heads, dim), bf),
            jax.ShapeDtypeStruct((tok * GROUPS, dim), bf),
            jax.ShapeDtypeStruct((tok * GROUPS, dim), bf),
        ),
        in_specs=[anywhere] * 4 + [pl.BlockSpec(memory_space=pltpu.SMEM)],
        out_specs=(anywhere,) * 3,
        scratch_shapes=[
            pltpu.VMEM((tok, heads, dim), bf),
            pltpu.VMEM((tok, heads, dim), bf),
            pltpu.VMEM((tok * GROUPS, dim), bf),
            pltpu.VMEM((tok * GROUPS, dim), bf),
            pltpu.VMEM((2, tok * GROUPS, dim), f32),
            pltpu.VMEM((GROUPS, 2, SLOTS * tok, dim), bf),
            pltpu.VMEM((GROUPS, qrows, dim), bf),
            pltpu.VMEM((GROUPS, dim, qrows), bf),
            pltpu.VMEM((GROUPS, qrows, dim), bf),
            pltpu.VMEM((GROUPS, dim, qrows), bf),
            pltpu.VMEM((1, qrows), jnp.int32),
            pltpu.VMEM((1, qrows), jnp.int32),
            pltpu.VMEM((GROUPS, SLOTS, qrows), f32),
            pltpu.VMEM((GROUPS, qrows), f32),
            pltpu.VMEM((GROUPS, qrows), f32),
            pltpu.VMEM((GROUPS, SLOTS * tok, qrows), f32),
            pltpu.VMEM((GROUPS, SLOTS * tok, qrows), f32),
            pltpu.VMEM((8, 128), bf),
            pltpu.VMEM((GROUPS, SLOTS * tok, qrows), bf),
            pltpu.VMEM((SLOTS, 4, tok, dim), f32),
            pltpu.VMEM((SLOTS - 1, 4, tok, dim), bf),
            pltpu.VMEM((SLOTS - 1, 4, tok, dim), bf),
            pltpu.VMEM((GROUPS, qrows, dim), f32),
            pltpu.VMEM((tok * GROUPS, dim), bf),
            pltpu.VMEM((tok * GROUPS, dim), bf),
            pltpu.VMEM((tok, heads, dim), bf),
            pltpu.SemaphoreType.DMA((4,)),
            pltpu.SemaphoreType.DMA((3,)),
            pltpu.SemaphoreType.DMA((SLOTS - 1, 4)),
            pltpu.SemaphoreType.DMA((SLOTS - 1, 4)),
            pltpu.SemaphoreType.DMA((SLOTS - 1, 4)),
            pltpu.SemaphoreType.DMA((SLOTS - 1, 4)),
        ],
        compiler_params=pltpu.CompilerParams(
            collective_id=0, has_side_effects=True, vmem_limit_bytes=67_043_328
        ),
    )(
        queries,
        key_vectors.reshape(tok * GROUPS, dim),
        value_matrix.reshape(tok * GROUPS, dim),
        grad_out,
        doc_lengths,
    )
    return dq, dk.reshape(tok, GROUPS, dim), dv.reshape(tok, GROUPS, dim)


def solution(mesh):
    spec = P("ctx", "tp", None)
    return jax.shard_map(
        functools.partial(local, mesh.shape["ctx"]),
        mesh=mesh,
        in_specs=(spec, spec, spec, spec, P()),
        out_specs=(spec, spec, spec),
        check_vma=False,
    )
```

```python
import functools

import jax
import jax.numpy as jnp
from jax import lax
from jax.experimental import pallas as pl
from jax.experimental.pallas import tpu as pltpu
from jax.sharding import PartitionSpec as P

RING = 4
SLOTS = 8
FAN = 8
DIM = 128
QTILE = 256
GROUPS = 2
LOG2E = 1.4426950408889634
DEAD = -1e30


KINDS = ("A", "P", "F", "S", "B", "R", "Q", "O")
ORDER = (
    0, 1, 2, 3, 100, 201, 40, 200, 41, 10, 240, 11, 42, 210, 30, 31, 12, 230,
    43, 50, 32, 241, 51, 250, 70, 33, 231, 13, 71, 211, 21, 20, 220, 60, 52, 270,
    61, 260, 300, 72, 460, 561, 450, 73, 420, 520, 470, 53, 560, 271, 22, 430, 521, 571,
    62, 251, 63, 550, 261, 570, 23, 221, 301, 461, 563, 562, 551, 421, 523, 522, 401, 440,
    471, 573, 531, 451, 553, 410, 511, 572, 431, 552, 530, 441, 411, 510, 400, 630, 533, 541,
    540, 640, 601, 600, 513, 532, 621, 543, 512, 611, 542, 650, 500, 610, 641, 631, 651, 620,
    700, 501, 503, 502,
)


def kernel(
    tok, nctx, ndocs, q_hbm, k_hbm, v_hbm, do_hbm, len_ref, dq_ref, dk_ref, dv_ref,
    qin, doin, kin, vin, wide, kv, qrow, qcol, orow, ocol, start_ref, pos_ref,
    mst, lst, dst_, prob, gprob, dscore, grad, sbuf, rbuf, dqf,
    in_sem, fs_sem, fr_sem, rs_sem, rr_sem,
):
    me = lax.axis_index("ctx")
    y = lax.rem(me, RING)
    row = me - y
    up = row + lax.rem(y + 1, RING)
    down = row + lax.rem(y + RING - 1, RING)
    ahead = lax.rem(me + RING, nctx)
    behind = lax.rem(me + nctx - RING, nctx)
    qrows = tok * FAN
    tiles = qrows // QTILE
    scale = DIM**-0.5

    copies = [
        pltpu.make_async_copy(k_hbm, kin, in_sem.at[0]),
        pltpu.make_async_copy(v_hbm, vin, in_sem.at[1]),
        pltpu.make_async_copy(q_hbm, qin, in_sem.at[2]),
        pltpu.make_async_copy(do_hbm, doin, in_sem.at[3]),
    ]
    for copy in copies:
        copy.start()
    barrier = pltpu.get_barrier_semaphore()
    for other in (up, down, ahead, behind):
        pl.semaphore_signal(
            barrier, inc=1, device_id={"ctx": other}, device_id_type=pl.DeviceIdType.MESH
        )
    for which, source in enumerate((kin, vin)):
        copies[which].wait()
        wide[which] = source[...].astype(jnp.float32)
        for g in range(GROUPS):
            kv[g, which, 0:tok] = wide[which, pl.ds(g, tok, stride=GROUPS), :].astype(jnp.bfloat16)
    pl.semaphore_wait(barrier, 4)

    fetch = {
        1: (up, jnp.where(y < RING - 1, 0, 4)),
        2: (up, jnp.where(y < RING - 1, 1, 5)),
        3: (down, jnp.where(y > 0, 4, 0)),
        4: (ahead, 0),
        5: (ahead, 1),
        6: (down, jnp.where(y > 0, 7, 3)),
        7: (ahead, 3),
    }
    parent = {1: down, 2: down, 3: up, 4: behind, 5: behind, 6: up, 7: behind}

    def fetch_copy(slot, c):
        target, source = fetch[slot]
        g, which = c // 2, c % 2
        rows = pl.ds(pl.multiple_of(source * tok, 16), tok)
        return pltpu.make_async_remote_copy(
            src_ref=kv.at[g, which, rows],
            dst_ref=kv.at[g, which, pl.ds(slot * tok, tok)],
            send_sem=fs_sem.at[slot - 1, c],
            recv_sem=fr_sem.at[slot - 1, c],
            device_id={"ctx": target},
            device_id_type=pl.DeviceIdType.MESH,
        )

    def return_copy(slot, c):
        return pltpu.make_async_remote_copy(
            src_ref=sbuf.at[slot - 1, c],
            dst_ref=rbuf.at[slot - 1, c],
            send_sem=rs_sem.at[slot - 1, c],
            recv_sem=rr_sem.at[slot - 1, c],
            device_id={"ctx": parent[slot]},
            device_id_type=pl.DeviceIdType.MESH,
        )

    def start_if(condition, slot, c):
        if condition is None:
            fetch_copy(slot, c).start()
        else:

            @pl.when(condition)
            def _():
                fetch_copy(slot, c).start()

    forwards = {
        0: ((4, None), (1, y < RING - 1), (3, y == 0)),
        1: ((5, None), (2, y < RING - 1)),
        4: ((1, y == RING - 1), (3, y > 0)),
        3: ((7, None), (6, y == 0)),
        5: ((2, y == RING - 1),),
        7: ((6, y > 0),),
        2: (),
        6: (),
    }

    def arrive(slot, c):
        if slot > 0:
            fetch_copy(slot, c).wait_recv()
        for onward, condition in forwards[slot]:
            start_if(condition, onward, c)

    step = QTILE // FAN

    def prepare():
        sources = ((qin, qrow, qcol), (doin, orow, ocol))
        for which, (source, rows_ref, cols_ref) in enumerate(sources):
            copies[2 + which].wait()

            @pl.loop(0, tok // step)
            def _(n):
                block = source[pl.ds(n * step, step)].astype(jnp.float32)
                at = pl.ds(pl.multiple_of(n * QTILE, QTILE), QTILE)
                for g in range(GROUPS):
                    part = block[:, g * FAN : (g + 1) * FAN, :].reshape(QTILE, DIM)
                    rows_ref[g, at, :] = part.astype(jnp.bfloat16)
                    cols_ref[g, :, at] = part.T.astype(jnp.bfloat16)

        pos = lax.broadcasted_iota(jnp.int32, (1, qrows), 1)
        pos = me * tok + lax.shift_right_logical(pos, 3)

        def doc_step(n, carried):
            end, begin = carried
            end = end + len_ref[n]
            return end, jnp.where(pos >= end, end, begin)

        empty = (jnp.int32(0), jnp.zeros_like(pos))
        unused, begin = lax.fori_loop(0, ndocs, doc_step, empty)
        start_ref[...] = begin
        pos_ref[...] = pos

    last = {0: None, 1: None}

    def first_pass(slot, g):
        rows = slice(slot * tok, (slot + 1) * tok)
        keys, values = kv[g, 0, rows], kv[g, 1, rows]
        before = last[g]
        key_pos = (me - slot) * tok + lax.broadcasted_iota(jnp.int32, (tok, QTILE), 0)
        for n in range(tiles):
            at = slice(n * QTILE, (n + 1) * QTILE)
            scores = jnp.dot(keys, qcol[g, :, at], preferred_element_type=jnp.float32)
            grads = jnp.dot(values, ocol[g, :, at], preferred_element_type=jnp.float32)
            live = key_pos >= start_ref[:, at]
            if slot == 0:
                live = live & (key_pos <= pos_ref[:, at])
            scores = jnp.where(live, scores * (scale * LOG2E), DEAD)
            top = jnp.max(scores, axis=0, keepdims=True)
            if before is not None:
                old = mst[g, before : before + 1, at]
                top = jnp.maximum(top, old)
            probs = jnp.exp2(scores - top)
            total = jnp.sum(probs, axis=0, keepdims=True)
            dots = jnp.sum(probs * grads, axis=0, keepdims=True)
            if before is not None:
                shrink = jnp.exp2(old - top)
                total = total + lst[g : g + 1, at] * shrink
                dots = dots + dst_[g : g + 1, at] * shrink
            mst[g, slot : slot + 1, at] = top
            lst[g : g + 1, at] = total
            dst_[g : g + 1, at] = dots
            prob[g, rows, at] = probs
            gprob[g, rows, at] = grads
        last[g] = slot

    def statistics(g):
        inverse = 1.0 / lst[g : g + 1, :]
        final = mst[g, last[g] : last[g] + 1, :]
        dst_[g : g + 1, :] = dst_[g : g + 1, :] * inverse
        for slot in range(SLOTS):
            mst[g, slot : slot + 1, :] = jnp.exp2(mst[g, slot : slot + 1, :] - final) * inverse

    def second_pass(slot, g):
        rows = slice(slot * tok, (slot + 1) * tok)
        key_sum, value_sum = None, None
        for n in range(tiles):
            at = slice(n * QTILE, (n + 1) * QTILE)
            probs = prob[g, rows, at] * mst[g, slot : slot + 1, at]
            scores = probs * (gprob[g, rows, at] - dst_[g : g + 1, at])
            low, scores = probs.astype(jnp.bfloat16), scores.astype(jnp.bfloat16)
            dscore[g, rows, at] = scores
            value_part = jnp.dot(low, orow[g, at, :], preferred_element_type=jnp.float32)
            key_part = jnp.dot(scores, qrow[g, at, :], preferred_element_type=jnp.float32)
            key_sum = key_part if n == 0 else key_sum + key_part
            value_sum = value_part if n == 0 else value_sum + value_part
        if slot in (2, 6):
            sbuf[slot - 1, 2 * g] = key_sum.astype(jnp.bfloat16)
            sbuf[slot - 1, 2 * g + 1] = value_sum.astype(jnp.bfloat16)
        else:
            grad[slot, 2 * g] = key_sum
            grad[slot, 2 * g + 1] = value_sum

    takes = {
        7: ((6, y > 0),),
        5: ((2, y == RING - 1),),
        3: ((7, None), (6, y == 0)),
        1: ((5, None), (2, y < RING - 1)),
        4: ((1, y == RING - 1), (3, y > 0)),
        0: ((4, None), (1, y < RING - 1), (3, y == 0)),
    }

    def take(slot, given, c):
        return_copy(given, c).wait_recv()
        grad[slot, c] = grad[slot, c] + rbuf[given - 1, c].astype(jnp.float32)

    def give_back(slot, c):
        for given, condition in takes.get(slot, ()):
            if condition is None:
                take(slot, given, c)
            else:
                pl.when(condition)(functools.partial(take, slot, given, c))
        if slot in takes and slot > 0:
            sbuf[slot - 1, c] = grad[slot, c].astype(jnp.bfloat16)
        if slot > 0:
            return_copy(slot, c).start()

    def query_grads(n, g):
        at = slice(n * QTILE, (n + 1) * QTILE)
        part = lax.dot_general(
            dscore[g, :, at], kv[g, 0], (((0,), (0,)), ((), ())),
            preferred_element_type=jnp.float32,
        )
        dqf[g, at, :] = part * scale

    def write_queries():
        @pl.loop(0, tok // step)
        def _(n):
            at = pl.ds(pl.multiple_of(n * QTILE, QTILE), QTILE)
            parts = [dqf[g, at, :].reshape(step, FAN, DIM) for g in range(GROUPS)]
            dq_ref[pl.ds(n * step, step)] = jnp.concatenate(parts, axis=1).astype(jnp.bfloat16)

    acts = {
        "P": lambda unused, none: prepare(), "A": arrive, "F": first_pass, "B": second_pass,
        "S": lambda unused, g: statistics(g), "Q": query_grads, "R": give_back,
        "O": lambda unused, none: write_queries(),
    }
    for code in ORDER:
        kind, rest = KINDS[code // 100], code % 100
        if kind != "Q" or rest // 10 < tiles:
            acts[kind](rest // 10, rest % 10)

    for g in range(GROUPS):
        wide[0, pl.ds(g, tok, stride=GROUPS), :] = grad[0, 2 * g] * scale
        wide[1, pl.ds(g, tok, stride=GROUPS), :] = grad[0, 2 * g + 1]
    dk_ref[...] = wide[0].astype(jnp.bfloat16)
    dv_ref[...] = wide[1].astype(jnp.bfloat16)
    for slot in range(1, SLOTS):
        for c in range(4):
            fetch_copy(slot, c).wait_send()
            return_copy(slot, c).wait_send()


def writer(a, b, c, out_a, out_b, out_c, sem):
    pairs = ((a, out_a), (b, out_b), (c, out_c))
    copies = [pltpu.make_async_copy(x, o, sem.at[i]) for i, (x, o) in enumerate(pairs)]
    for copy in copies:
        copy.start()
    for copy in copies:
        copy.wait()

def local(nctx, queries, key_vectors, value_matrix, grad_out, doc_lengths):
    tok, heads, dim = queries.shape
    qrows = tok * FAN
    bf, f32 = jnp.bfloat16, jnp.float32
    anywhere = pl.BlockSpec(memory_space=pl.ANY)
    shapes = ((tok, heads, dim), (tok * GROUPS, dim), (tok * GROUPS, dim))
    inside = pl.BlockSpec(memory_space=pltpu.VMEM)
    parts = pl.pallas_call(
        functools.partial(kernel, tok, nctx, doc_lengths.shape[0]),
        out_shape=tuple(pltpu.VMEM(shape, bf) for shape in shapes),
        in_specs=[anywhere] * 4 + [pl.BlockSpec(memory_space=pltpu.SMEM)],
        out_specs=(inside,) * 3,
        scratch_shapes=[
            pltpu.VMEM((tok, heads, dim), bf),
            pltpu.VMEM((tok, heads, dim), bf),
            pltpu.VMEM((tok * GROUPS, dim), bf),
            pltpu.VMEM((tok * GROUPS, dim), bf),
            pltpu.VMEM((2, tok * GROUPS, dim), f32),
            pltpu.VMEM((GROUPS, 2, SLOTS * tok, dim), bf),
            pltpu.VMEM((GROUPS, qrows, dim), bf),
            pltpu.VMEM((GROUPS, dim, qrows), bf),
            pltpu.VMEM((GROUPS, qrows, dim), bf),
            pltpu.VMEM((GROUPS, dim, qrows), bf),
            pltpu.VMEM((1, qrows), jnp.int32),
            pltpu.VMEM((1, qrows), jnp.int32),
            pltpu.VMEM((GROUPS, SLOTS, qrows), f32),
            pltpu.VMEM((GROUPS, qrows), f32),
            pltpu.VMEM((GROUPS, qrows), f32),
            pltpu.VMEM((GROUPS, SLOTS * tok, qrows), f32),
            pltpu.VMEM((GROUPS, SLOTS * tok, qrows), f32),
            pltpu.VMEM((GROUPS, SLOTS * tok, qrows), bf),
            pltpu.VMEM((SLOTS, 4, tok, dim), f32),
            pltpu.VMEM((SLOTS - 1, 4, tok, dim), bf),
            pltpu.VMEM((SLOTS - 1, 4, tok, dim), bf),
            pltpu.VMEM((GROUPS, qrows, dim), f32),
            pltpu.SemaphoreType.DMA((4,)),
            pltpu.SemaphoreType.DMA((SLOTS - 1, 4)),
            pltpu.SemaphoreType.DMA((SLOTS - 1, 4)),
            pltpu.SemaphoreType.DMA((SLOTS - 1, 4)),
            pltpu.SemaphoreType.DMA((SLOTS - 1, 4)),
        ],
        compiler_params=pltpu.CompilerParams(
            collective_id=0, has_side_effects=True, vmem_limit_bytes=63_000_000
        ),
    )(
        queries,
        key_vectors.reshape(tok * GROUPS, dim),
        value_matrix.reshape(tok * GROUPS, dim),
        grad_out,
        doc_lengths,
    )
    dq, dk, dv = pl.pallas_call(
        writer,
        out_shape=tuple(jax.ShapeDtypeStruct(shape, bf) for shape in shapes),
        in_specs=[anywhere] * 3,
        out_specs=(anywhere,) * 3,
        scratch_shapes=[pltpu.SemaphoreType.DMA((3,))],
        compiler_params=pltpu.CompilerParams(vmem_limit_bytes=1_000_000),
    )(*[pltpu.with_memory_space_constraint(part, pltpu.VMEM) for part in parts])
    return dq, dk.reshape(tok, GROUPS, dim), dv.reshape(tok, GROUPS, dim)


def solution(mesh):
    spec = P("ctx", "tp", None)
    return jax.shard_map(
        functools.partial(local, mesh.shape["ctx"]),
        mesh=mesh,
        in_specs=(spec, spec, spec, spec, P()),
        out_specs=(spec, spec, spec),
        check_vma=False,
    )
```

```python
import functools

import jax
import jax.numpy as jnp
from jax import lax
from jax.experimental import pallas as pl
from jax.experimental.pallas import tpu as pltpu
from jax.sharding import PartitionSpec as P

RING = 4
SLOTS = 8
RELAY = 8
FAN = 8
DIM = 128
QTILE = 256
GROUPS = 2
LOG2E = 1.4426950408889634
DEAD = -1e30


KINDS = ("A", "P", "F", "S", "B", "R", "Q", "O")
ORDER = (
    0, 1, 2, 3, 100, 201, 200, 40, 41, 240, 42, 11, 43, 10, 241, 31, 30, 12,
    80, 210, 82, 32, 13, 211, 33, 50, 231, 51, 230, 71, 70, 270, 250, 52, 20, 72,
    53, 251, 21, 220, 73, 271, 61, 60, 260, 22, 300, 460, 561, 420, 62, 521, 470, 560,
    63, 520, 23, 261, 221, 301, 421, 523, 461, 562, 571, 450, 551, 522, 563, 451, 471, 550,
    570, 440, 411, 553, 572, 400, 552, 430, 573, 531, 410, 600, 511, 530, 580, 510, 431, 620,
    532, 582, 512, 630, 533, 541, 513, 540, 441, 401, 542, 640, 631, 543, 501, 601, 610, 650,
    621, 641, 500, 651, 502, 611, 700, 503,
)


def kernel(
    tok, nctx, ndocs, q_hbm, k_hbm, v_hbm, do_hbm, len_ref, dq_ref, dk_ref, dv_ref,
    qin, doin, kin, vin, wide, kv, qrow, qcol, orow, ocol, start_ref, pos_ref,
    mst, lst, dst_, prob, gprob, dscore, grad, sbuf, rbuf, dqf,
    in_sem, fs_sem, fr_sem, rs_sem, rr_sem,
):
    me = lax.axis_index("ctx")
    y = lax.rem(me, RING)
    row = me - y
    up = row + lax.rem(y + 1, RING)
    down = row + lax.rem(y + RING - 1, RING)
    ahead = lax.rem(me + RING, nctx)
    behind = lax.rem(me + nctx - RING, nctx)
    qrows = tok * FAN
    tiles = qrows // QTILE
    scale = DIM**-0.5

    copies = [
        pltpu.make_async_copy(k_hbm, kin, in_sem.at[0]),
        pltpu.make_async_copy(v_hbm, vin, in_sem.at[1]),
        pltpu.make_async_copy(q_hbm, qin, in_sem.at[2]),
        pltpu.make_async_copy(do_hbm, doin, in_sem.at[3]),
    ]
    for copy in copies:
        copy.start()
    barrier = pltpu.get_barrier_semaphore()
    for other in (up, down, ahead, behind):
        pl.semaphore_signal(
            barrier, inc=1, device_id={"ctx": other}, device_id_type=pl.DeviceIdType.MESH
        )
    for which, source in enumerate((kin, vin)):
        copies[which].wait()
        wide[which] = source[...].astype(jnp.float32)
        for g in range(GROUPS):
            kv[g, which, 0:tok] = wide[which, pl.ds(g, tok, stride=GROUPS), :].astype(jnp.bfloat16)
    pl.semaphore_wait(barrier, 4)

    common = {
        1: (up, jnp.where(y < RING - 1, 0, 4)),
        2: (up, jnp.where(y < RING - 1, 1, 5)),
        3: (down, jnp.where(y > 0, 4, 0)),
        4: (ahead, 0),
        6: (down, jnp.where(y > 0, 7, 3)),
    }
    key_tree = {
        5: (up, jnp.where(y < RING - 1, 4, RELAY)),
        7: (down, jnp.where(y > 0, RELAY, 4)),
        RELAY: (ahead, 4),
    }
    fetch = (common | key_tree, common | {5: (ahead, 1), 7: (ahead, 3)})
    upper = {1: down, 2: down, 3: up, 4: behind, 6: up}
    parent = (upper | {5: down, 7: up, RELAY: behind}, upper | {5: behind, 7: behind})

    def fetch_copy(slot, c):
        g, which = c // 2, c % 2
        target, source = fetch[which][slot]
        rows = pl.ds(pl.multiple_of(source * tok, 16), tok)
        return pltpu.make_async_remote_copy(
            src_ref=kv.at[g, which, rows],
            dst_ref=kv.at[g, which, pl.ds(slot * tok, tok)],
            send_sem=fs_sem.at[slot - 1, c],
            recv_sem=fr_sem.at[slot - 1, c],
            device_id={"ctx": target},
            device_id_type=pl.DeviceIdType.MESH,
        )

    def return_copy(slot, c):
        return pltpu.make_async_remote_copy(
            src_ref=sbuf.at[slot - 1, c],
            dst_ref=rbuf.at[slot - 1, c],
            send_sem=rs_sem.at[slot - 1, c],
            recv_sem=rr_sem.at[slot - 1, c],
            device_id={"ctx": parent[c % 2][slot]},
            device_id_type=pl.DeviceIdType.MESH,
        )

    def start_if(condition, slot, c):
        if condition is None:
            fetch_copy(slot, c).start()
        else:

            @pl.when(condition)
            def _():
                fetch_copy(slot, c).start()

    first = ((4, None), (1, y < RING - 1), (3, y == 0))
    forwards = (
        {
            0: first,
            1: ((2, y < RING - 1),),
            4: (
                (RELAY, y > 0), (1, y == RING - 1), (3, y > 0),
                (5, y < RING - 1), (7, y == 0),
            ),
            3: ((6, y == 0),),
            5: ((2, y == RING - 1),),
            7: ((6, y > 0),),
            RELAY: ((5, y == RING - 1), (7, y > 0)),
            2: (),
            6: (),
        },
        {
            0: first,
            1: ((5, None), (2, y < RING - 1)),
            4: ((1, y == RING - 1), (3, y > 0)),
            3: ((7, None), (6, y == 0)),
            5: ((2, y == RING - 1),),
            7: ((6, y > 0),),
            2: (),
            6: (),
        },
    )

    def arrive(slot, c):
        if slot == RELAY:

            @pl.when(y > 0)
            def _():
                fetch_copy(slot, c).wait_recv()

        elif slot > 0:
            fetch_copy(slot, c).wait_recv()
        for onward, condition in forwards[c % 2][slot]:
            start_if(condition, onward, c)

    step = QTILE // FAN

    def prepare():
        sources = ((qin, qrow, qcol), (doin, orow, ocol))
        for which, (source, rows_ref, cols_ref) in enumerate(sources):
            copies[2 + which].wait()

            @pl.loop(0, tok // step)
            def _(n):
                block = source[pl.ds(n * step, step)].astype(jnp.float32)
                at = pl.ds(pl.multiple_of(n * QTILE, QTILE), QTILE)
                for g in range(GROUPS):
                    part = block[:, g * FAN : (g + 1) * FAN, :].reshape(QTILE, DIM)
                    rows_ref[g, at, :] = part.astype(jnp.bfloat16)
                    cols_ref[g, :, at] = part.T.astype(jnp.bfloat16)

        pos = lax.broadcasted_iota(jnp.int32, (1, qrows), 1)
        pos = me * tok + lax.shift_right_logical(pos, 3)

        def doc_step(n, carried):
            end, begin = carried
            end = end + len_ref[n]
            return end, jnp.where(pos >= end, end, begin)

        empty = (jnp.int32(0), jnp.zeros_like(pos))
        unused, begin = lax.fori_loop(0, ndocs, doc_step, empty)
        start_ref[...] = begin
        pos_ref[...] = pos

    last = {0: None, 1: None}

    def first_pass(slot, g):
        rows = slice(slot * tok, (slot + 1) * tok)
        keys, values = kv[g, 0, rows], kv[g, 1, rows]
        before = last[g]
        key_pos = (me - slot) * tok + lax.broadcasted_iota(jnp.int32, (tok, QTILE), 0)
        for n in range(tiles):
            at = slice(n * QTILE, (n + 1) * QTILE)
            scores = jnp.dot(keys, qcol[g, :, at], preferred_element_type=jnp.float32)
            grads = jnp.dot(values, ocol[g, :, at], preferred_element_type=jnp.float32)
            live = key_pos >= start_ref[:, at]
            if slot == 0:
                live = live & (key_pos <= pos_ref[:, at])
            scores = jnp.where(live, scores * (scale * LOG2E), DEAD)
            top = jnp.max(scores, axis=0, keepdims=True)
            if before is not None:
                old = mst[g, before : before + 1, at]
                top = jnp.maximum(top, old)
            probs = jnp.exp2(scores - top)
            total = jnp.sum(probs, axis=0, keepdims=True)
            dots = jnp.sum(probs * grads, axis=0, keepdims=True)
            if before is not None:
                shrink = jnp.exp2(old - top)
                total = total + lst[g : g + 1, at] * shrink
                dots = dots + dst_[g : g + 1, at] * shrink
            mst[g, slot : slot + 1, at] = top
            lst[g : g + 1, at] = total
            dst_[g : g + 1, at] = dots
            prob[g, rows, at] = probs
            gprob[g, rows, at] = grads
        last[g] = slot

    def statistics(g):
        inverse = 1.0 / lst[g : g + 1, :]
        final = mst[g, last[g] : last[g] + 1, :]
        dst_[g : g + 1, :] = dst_[g : g + 1, :] * inverse
        for slot in range(SLOTS):
            mst[g, slot : slot + 1, :] = jnp.exp2(mst[g, slot : slot + 1, :] - final) * inverse

    def second_pass(slot, g):
        rows = slice(slot * tok, (slot + 1) * tok)
        key_sum, value_sum = None, None
        for n in range(tiles):
            at = slice(n * QTILE, (n + 1) * QTILE)
            probs = prob[g, rows, at] * mst[g, slot : slot + 1, at]
            scores = probs * (gprob[g, rows, at] - dst_[g : g + 1, at])
            low, scores = probs.astype(jnp.bfloat16), scores.astype(jnp.bfloat16)
            dscore[g, rows, at] = scores
            value_part = jnp.dot(low, orow[g, at, :], preferred_element_type=jnp.float32)
            key_part = jnp.dot(scores, qrow[g, at, :], preferred_element_type=jnp.float32)
            key_sum = key_part if n == 0 else key_sum + key_part
            value_sum = value_part if n == 0 else value_sum + value_part
        if slot in (2, 6):
            sbuf[slot - 1, 2 * g] = key_sum.astype(jnp.bfloat16)
            sbuf[slot - 1, 2 * g + 1] = value_sum.astype(jnp.bfloat16)
        else:
            grad[slot, 2 * g] = key_sum
            grad[slot, 2 * g + 1] = value_sum

    def take(slot, given, c):
        return_copy(given, c).wait_recv()
        grad[slot, c] = grad[slot, c] + rbuf[given - 1, c].astype(jnp.float32)

    def give_back(slot, c):
        taken = forwards[c % 2][slot]
        if slot == RELAY:
            grad[slot, c] = jnp.zeros((tok, DIM), jnp.float32)
        for given, condition in taken:
            if condition is None:
                take(slot, given, c)
            else:
                pl.when(condition)(functools.partial(take, slot, given, c))
        if taken and slot > 0:
            sbuf[slot - 1, c] = grad[slot, c].astype(jnp.bfloat16)
        if slot == RELAY:

            @pl.when(y > 0)
            def _():
                return_copy(slot, c).start()

        elif slot > 0:
            return_copy(slot, c).start()

    def query_grads(n, g):
        at = slice(n * QTILE, (n + 1) * QTILE)
        part = lax.dot_general(
            dscore[g, :, at], kv[g, 0, 0 : SLOTS * tok], (((0,), (0,)), ((), ())),
            preferred_element_type=jnp.float32,
        )
        dqf[g, at, :] = part * scale

    def write_queries():
        @pl.loop(0, tok // step)
        def _(n):
            at = pl.ds(pl.multiple_of(n * QTILE, QTILE), QTILE)
            parts = [dqf[g, at, :].reshape(step, FAN, DIM) for g in range(GROUPS)]
            dq_ref[pl.ds(n * step, step)] = jnp.concatenate(parts, axis=1).astype(jnp.bfloat16)

    acts = {
        "P": lambda unused, none: prepare(), "A": arrive, "F": first_pass, "B": second_pass,
        "S": lambda unused, g: statistics(g), "Q": query_grads, "R": give_back,
        "O": lambda unused, none: write_queries(),
    }
    for code in ORDER:
        kind, rest = KINDS[code // 100], code % 100
        if kind != "Q" or rest // 10 < tiles:
            acts[kind](rest // 10, rest % 10)

    for g in range(GROUPS):
        wide[0, pl.ds(g, tok, stride=GROUPS), :] = grad[0, 2 * g] * scale
        wide[1, pl.ds(g, tok, stride=GROUPS), :] = grad[0, 2 * g + 1]
    dk_ref[...] = wide[0].astype(jnp.bfloat16)
    dv_ref[...] = wide[1].astype(jnp.bfloat16)
    for slot in range(1, SLOTS):
        for c in range(4):
            fetch_copy(slot, c).wait_send()
            return_copy(slot, c).wait_send()

    @pl.when(y > 0)
    def _():
        for c in (0, 2):
            fetch_copy(RELAY, c).wait_send()
            return_copy(RELAY, c).wait_send()


def writer(a, b, c, out_a, out_b, out_c, sem):
    pairs = ((a, out_a), (b, out_b), (c, out_c))
    copies = [pltpu.make_async_copy(x, o, sem.at[i]) for i, (x, o) in enumerate(pairs)]
    for copy in copies:
        copy.start()
    for copy in copies:
        copy.wait()

def local(nctx, queries, key_vectors, value_matrix, grad_out, doc_lengths):
    tok, heads, dim = queries.shape
    qrows = tok * FAN
    bf, f32 = jnp.bfloat16, jnp.float32
    anywhere = pl.BlockSpec(memory_space=pl.ANY)
    shapes = ((tok, heads, dim), (tok * GROUPS, dim), (tok * GROUPS, dim))
    inside = pl.BlockSpec(memory_space=pltpu.VMEM)
    parts = pl.pallas_call(
        functools.partial(kernel, tok, nctx, doc_lengths.shape[0]),
        out_shape=tuple(pltpu.VMEM(shape, bf) for shape in shapes),
        in_specs=[anywhere] * 4 + [pl.BlockSpec(memory_space=pltpu.SMEM)],
        out_specs=(inside,) * 3,
        scratch_shapes=[
            pltpu.VMEM((tok, heads, dim), bf),
            pltpu.VMEM((tok, heads, dim), bf),
            pltpu.VMEM((tok * GROUPS, dim), bf),
            pltpu.VMEM((tok * GROUPS, dim), bf),
            pltpu.VMEM((2, tok * GROUPS, dim), f32),
            pltpu.VMEM((GROUPS, 2, (SLOTS + 1) * tok, dim), bf),
            pltpu.VMEM((GROUPS, qrows, dim), bf),
            pltpu.VMEM((GROUPS, dim, qrows), bf),
            pltpu.VMEM((GROUPS, qrows, dim), bf),
            pltpu.VMEM((GROUPS, dim, qrows), bf),
            pltpu.VMEM((1, qrows), jnp.int32),
            pltpu.VMEM((1, qrows), jnp.int32),
            pltpu.VMEM((GROUPS, SLOTS, qrows), f32),
            pltpu.VMEM((GROUPS, qrows), f32),
            pltpu.VMEM((GROUPS, qrows), f32),
            pltpu.VMEM((GROUPS, SLOTS * tok, qrows), f32),
            pltpu.VMEM((GROUPS, SLOTS * tok, qrows), f32),
            pltpu.VMEM((GROUPS, SLOTS * tok, qrows), bf),
            pltpu.VMEM((SLOTS + 1, 4, tok, dim), f32),
            pltpu.VMEM((SLOTS, 4, tok, dim), bf),
            pltpu.VMEM((SLOTS, 4, tok, dim), bf),
            pltpu.VMEM((GROUPS, qrows, dim), f32),
            pltpu.SemaphoreType.DMA((4,)),
            pltpu.SemaphoreType.DMA((SLOTS, 4)),
            pltpu.SemaphoreType.DMA((SLOTS, 4)),
            pltpu.SemaphoreType.DMA((SLOTS, 4)),
            pltpu.SemaphoreType.DMA((SLOTS, 4)),
        ],
        compiler_params=pltpu.CompilerParams(
            collective_id=0, has_side_effects=True, vmem_limit_bytes=64_500_000
        ),
    )(
        queries,
        key_vectors.reshape(tok * GROUPS, dim),
        value_matrix.reshape(tok * GROUPS, dim),
        grad_out,
        doc_lengths,
    )
    dq, dk, dv = pl.pallas_call(
        writer,
        out_shape=tuple(jax.ShapeDtypeStruct(shape, bf) for shape in shapes),
        in_specs=[anywhere] * 3,
        out_specs=(anywhere,) * 3,
        scratch_shapes=[pltpu.SemaphoreType.DMA((3,))],
        compiler_params=pltpu.CompilerParams(vmem_limit_bytes=1_000_000),
    )(*[pltpu.with_memory_space_constraint(part, pltpu.VMEM) for part in parts])
    return dq, dk.reshape(tok, GROUPS, dim), dv.reshape(tok, GROUPS, dim)


def solution(mesh):
    spec = P("ctx", "tp", None)
    return jax.shard_map(
        functools.partial(local, mesh.shape["ctx"]),
        mesh=mesh,
        in_specs=(spec, spec, spec, spec, P()),
        out_specs=(spec, spec, spec),
        check_vma=False,
    )
```

```python
import functools

import jax
import jax.numpy as jnp
from jax import lax
from jax.experimental import pallas as pl
from jax.experimental.pallas import tpu as pltpu
from jax.sharding import PartitionSpec as P

RING = 4
SLOTS = 8
RELAY = 8
FAN = 8
DIM = 128
QTILE = 256
GROUPS = 2
LOG2E = 1.4426950408889634
DEAD = -1e30


KINDS = ("A", "P", "F", "S", "B", "R", "Q", "O")
ORDER = (
    0, 1, 2, 3, 100, 201, 200, 40, 41, 240, 42, 11, 43, 10, 241, 31, 30, 12,
    80, 210, 82, 32, 13, 211, 33, 50, 231, 51, 230, 71, 70, 270, 250, 52, 20, 72,
    53, 251, 21, 220, 73, 271, 61, 60, 260, 22, 300, 460, 561, 420, 62, 521, 470, 560,
    63, 520, 23, 261, 221, 301, 421, 523, 461, 562, 571, 450, 551, 522, 563, 451, 471, 550,
    570, 440, 411, 553, 572, 400, 552, 430, 573, 531, 410, 600, 511, 530, 580, 510, 431, 620,
    532, 582, 512, 630, 533, 541, 513, 540, 441, 401, 542, 640, 631, 543, 501, 601, 610, 650,
    621, 641, 500, 651, 502, 611, 700, 503,
)


def kernel(
    tok, nctx, ndocs, q_hbm, k_hbm, v_hbm, do_hbm, len_ref, dq_ref, dk_ref, dv_ref,
    qin, doin, kin, vin, wide, kv, qrow, qcol, orow, ocol, start_ref, pos_ref,
    mst, lst, dst_, prob, gprob, dscore, grad, sbuf, rbuf, dqf,
    in_sem, fs_sem, fr_sem, rs_sem, rr_sem,
):
    me = lax.axis_index("ctx")
    y = lax.rem(me, RING)
    row = me - y
    up = row + lax.rem(y + 1, RING)
    down = row + lax.rem(y + RING - 1, RING)
    ahead = lax.rem(me + RING, nctx)
    behind = lax.rem(me + nctx - RING, nctx)
    qrows = tok * FAN
    tiles = qrows // QTILE
    scale = DIM**-0.5

    copies = [
        pltpu.make_async_copy(k_hbm, kin, in_sem.at[0]),
        pltpu.make_async_copy(v_hbm, vin, in_sem.at[1]),
        pltpu.make_async_copy(q_hbm, qin, in_sem.at[2]),
        pltpu.make_async_copy(do_hbm, doin, in_sem.at[3]),
    ]
    for copy in copies:
        copy.start()
    barrier = pltpu.get_barrier_semaphore()
    for other in (up, down, ahead, behind):
        pl.semaphore_signal(
            barrier, inc=1, device_id={"ctx": other}, device_id_type=pl.DeviceIdType.MESH
        )
    for which, source in enumerate((kin, vin)):
        copies[which].wait()
        wide[which] = source[...].astype(jnp.float32)
        for g in range(GROUPS):
            kv[g, which, 0:tok] = wide[which, pl.ds(g, tok, stride=GROUPS), :].astype(jnp.bfloat16)
    pl.semaphore_wait(barrier, 4)

    common = {
        1: (up, jnp.where(y < RING - 1, 0, 4)),
        2: (up, jnp.where(y < RING - 1, 1, 5)),
        3: (down, jnp.where(y > 0, 4, 0)),
        4: (ahead, 0),
        6: (down, jnp.where(y > 0, 7, 3)),
    }
    key_tree = {
        5: (up, jnp.where(y < RING - 1, 4, RELAY)),
        7: (down, jnp.where(y > 0, RELAY, 4)),
        RELAY: (ahead, 4),
    }
    fetch = (common | key_tree, common | {5: (ahead, 1), 7: (ahead, 3)})
    upper = {1: down, 2: down, 3: up, 4: behind, 6: up}
    parent = (upper | {5: down, 7: up, RELAY: behind}, upper | {5: behind, 7: behind})

    def fetch_copy(slot, c):
        g, which = c // 2, c % 2
        target, source = fetch[which][slot]
        rows = pl.ds(pl.multiple_of(source * tok, 16), tok)
        return pltpu.make_async_remote_copy(
            src_ref=kv.at[g, which, rows],
            dst_ref=kv.at[g, which, pl.ds(slot * tok, tok)],
            send_sem=fs_sem.at[slot - 1, c],
            recv_sem=fr_sem.at[slot - 1, c],
            device_id={"ctx": target},
            device_id_type=pl.DeviceIdType.MESH,
        )

    def return_copy(slot, c):
        return pltpu.make_async_remote_copy(
            src_ref=sbuf.at[slot - 1, c],
            dst_ref=rbuf.at[slot - 1, c],
            send_sem=rs_sem.at[slot - 1, c],
            recv_sem=rr_sem.at[slot - 1, c],
            device_id={"ctx": parent[c % 2][slot]},
            device_id_type=pl.DeviceIdType.MESH,
        )

    def start_if(condition, slot, c):
        if condition is None:
            fetch_copy(slot, c).start()
        else:

            @pl.when(condition)
            def _():
                fetch_copy(slot, c).start()

    first = ((4, None), (1, y < RING - 1), (3, y == 0))
    forwards = (
        {
            0: first,
            1: ((2, y < RING - 1),),
            4: (
                (RELAY, y > 0), (1, y == RING - 1), (3, y > 0),
                (5, y < RING - 1), (7, y == 0),
            ),
            3: ((6, y == 0),),
            5: ((2, y == RING - 1),),
            7: ((6, y > 0),),
            RELAY: ((5, y == RING - 1), (7, y > 0)),
            2: (),
            6: (),
        },
        {
            0: first,
            1: ((5, None), (2, y < RING - 1)),
            4: ((1, y == RING - 1), (3, y > 0)),
            3: ((7, None), (6, y == 0)),
            5: ((2, y == RING - 1),),
            7: ((6, y > 0),),
            2: (),
            6: (),
        },
    )

    def arrive(slot, c):
        if slot == RELAY:

            @pl.when(y > 0)
            def _():
                fetch_copy(slot, c).wait_recv()

        elif slot > 0:
            fetch_copy(slot, c).wait_recv()
        for onward, condition in forwards[c % 2][slot]:
            start_if(condition, onward, c)

    step = QTILE // FAN

    def prepare():
        sources = ((qin, qrow, qcol), (doin, orow, ocol))
        for which, (source, rows_ref, cols_ref) in enumerate(sources):
            copies[2 + which].wait()

            @pl.loop(0, tok // step)
            def _(n):
                block = source[pl.ds(n * step, step)].astype(jnp.float32)
                at = pl.ds(pl.multiple_of(n * QTILE, QTILE), QTILE)
                for g in range(GROUPS):
                    part = block[:, g * FAN : (g + 1) * FAN, :].reshape(QTILE, DIM)
                    rows_ref[g, at, :] = part.astype(jnp.bfloat16)
                    cols_ref[g, :, at] = part.T.astype(jnp.bfloat16)

        pos = lax.broadcasted_iota(jnp.int32, (1, qrows), 1)
        pos = me * tok + lax.shift_right_logical(pos, 3)

        def doc_step(n, carried):
            end, begin = carried
            end = end + len_ref[n]
            return end, jnp.where(pos >= end, end, begin)

        empty = (jnp.int32(0), jnp.zeros_like(pos))
        unused, begin = lax.fori_loop(0, ndocs, doc_step, empty)
        start_ref[...] = begin
        pos_ref[...] = pos

    last = {0: None, 1: None}

    def first_pass(slot, g):
        before = last[g]
        for n in range(tiles):
            at = slice(n * QTILE, (n + 1) * QTILE)
            low, high = 0, tok
            if slot == 0:
                high = (n + 1) * step
            elif slot == SLOTS - 1:
                low = n * step
            rows = slice(slot * tok + low, slot * tok + high)
            scores = jnp.dot(kv[g, 0, rows], qcol[g, :, at], preferred_element_type=jnp.float32)
            grads = jnp.dot(kv[g, 1, rows], ocol[g, :, at], preferred_element_type=jnp.float32)
            key_pos = lax.broadcasted_iota(jnp.int32, (high - low, QTILE), 0)
            key_pos = key_pos + ((me - slot) * tok + low)
            live = key_pos >= start_ref[:, at]
            if slot == 0:
                live = live & (key_pos <= pos_ref[:, at])
            scores = jnp.where(live, scores * (scale * LOG2E), DEAD)
            top = jnp.max(scores, axis=0, keepdims=True)
            if before is not None:
                old = mst[g, before : before + 1, at]
                top = jnp.maximum(top, old)
            probs = jnp.exp2(scores - top)
            total = jnp.sum(probs, axis=0, keepdims=True)
            dots = jnp.sum(probs * grads, axis=0, keepdims=True)
            if before is not None:
                shrink = jnp.exp2(old - top)
                total = total + lst[g : g + 1, at] * shrink
                dots = dots + dst_[g : g + 1, at] * shrink
            mst[g, slot : slot + 1, at] = top
            lst[g : g + 1, at] = total
            dst_[g : g + 1, at] = dots
            prob[g, rows, at] = probs
            gprob[g, rows, at] = grads
            for start, stop in ((0, low), (high, tok)):
                if stop > start:
                    rest = slice(slot * tok + start, slot * tok + stop)
                    prob[g, rest, at] = jnp.zeros((stop - start, QTILE), jnp.float32)
                    gprob[g, rest, at] = jnp.zeros((stop - start, QTILE), jnp.float32)
        last[g] = slot

    def statistics(g):
        inverse = 1.0 / lst[g : g + 1, :]
        final = mst[g, last[g] : last[g] + 1, :]
        dst_[g : g + 1, :] = dst_[g : g + 1, :] * inverse
        for slot in range(SLOTS):
            mst[g, slot : slot + 1, :] = jnp.exp2(mst[g, slot : slot + 1, :] - final) * inverse

    def second_pass(slot, g):
        rows = slice(slot * tok, (slot + 1) * tok)
        key_sum, value_sum = None, None
        for n in range(tiles):
            at = slice(n * QTILE, (n + 1) * QTILE)
            probs = prob[g, rows, at] * mst[g, slot : slot + 1, at]
            scores = probs * (gprob[g, rows, at] - dst_[g : g + 1, at])
            low, scores = probs.astype(jnp.bfloat16), scores.astype(jnp.bfloat16)
            dscore[g, rows, at] = scores
            value_part = jnp.dot(low, orow[g, at, :], preferred_element_type=jnp.float32)
            key_part = jnp.dot(scores, qrow[g, at, :], preferred_element_type=jnp.float32)
            key_sum = key_part if n == 0 else key_sum + key_part
            value_sum = value_part if n == 0 else value_sum + value_part
        if slot in (2, 6):
            sbuf[slot - 1, 2 * g] = key_sum.astype(jnp.bfloat16)
            sbuf[slot - 1, 2 * g + 1] = value_sum.astype(jnp.bfloat16)
        else:
            grad[slot, 2 * g] = key_sum
            grad[slot, 2 * g + 1] = value_sum

    def take(slot, given, c):
        return_copy(given, c).wait_recv()
        grad[slot, c] = grad[slot, c] + rbuf[given - 1, c].astype(jnp.float32)

    def give_back(slot, c):
        taken = forwards[c % 2][slot]
        if slot == RELAY:
            grad[slot, c] = jnp.zeros((tok, DIM), jnp.float32)
        for given, condition in taken:
            if condition is None:
                take(slot, given, c)
            else:
                pl.when(condition)(functools.partial(take, slot, given, c))
        if taken and slot > 0:
            sbuf[slot - 1, c] = grad[slot, c].astype(jnp.bfloat16)
        if slot == RELAY:

            @pl.when(y > 0)
            def _():
                return_copy(slot, c).start()

        elif slot > 0:
            return_copy(slot, c).start()

    def query_grads(n, g):
        at = slice(n * QTILE, (n + 1) * QTILE)
        part = lax.dot_general(
            dscore[g, :, at], kv[g, 0, 0 : SLOTS * tok], (((0,), (0,)), ((), ())),
            preferred_element_type=jnp.float32,
        )
        dqf[g, at, :] = part * scale

    def write_queries():
        @pl.loop(0, tok // step)
        def _(n):
            at = pl.ds(pl.multiple_of(n * QTILE, QTILE), QTILE)
            parts = [dqf[g, at, :].reshape(step, FAN, DIM) for g in range(GROUPS)]
            dq_ref[pl.ds(n * step, step)] = jnp.concatenate(parts, axis=1).astype(jnp.bfloat16)

    acts = {
        "P": lambda unused, none: prepare(), "A": arrive, "F": first_pass, "B": second_pass,
        "S": lambda unused, g: statistics(g), "Q": query_grads, "R": give_back,
        "O": lambda unused, none: write_queries(),
    }
    for code in ORDER:
        kind, rest = KINDS[code // 100], code % 100
        if kind != "Q" or rest // 10 < tiles:
            acts[kind](rest // 10, rest % 10)

    for g in range(GROUPS):
        wide[0, pl.ds(g, tok, stride=GROUPS), :] = grad[0, 2 * g] * scale
        wide[1, pl.ds(g, tok, stride=GROUPS), :] = grad[0, 2 * g + 1]
    dk_ref[...] = wide[0].astype(jnp.bfloat16)
    dv_ref[...] = wide[1].astype(jnp.bfloat16)
    for slot in range(1, SLOTS):
        for c in range(4):
            fetch_copy(slot, c).wait_send()
            return_copy(slot, c).wait_send()

    @pl.when(y > 0)
    def _():
        for c in (0, 2):
            fetch_copy(RELAY, c).wait_send()
            return_copy(RELAY, c).wait_send()


def writer(a, b, c, out_a, out_b, out_c, sem):
    pairs = ((a, out_a), (b, out_b), (c, out_c))
    copies = [pltpu.make_async_copy(x, o, sem.at[i]) for i, (x, o) in enumerate(pairs)]
    for copy in copies:
        copy.start()
    for copy in copies:
        copy.wait()

def local(nctx, queries, key_vectors, value_matrix, grad_out, doc_lengths):
    tok, heads, dim = queries.shape
    qrows = tok * FAN
    bf, f32 = jnp.bfloat16, jnp.float32
    anywhere = pl.BlockSpec(memory_space=pl.ANY)
    shapes = ((tok, heads, dim), (tok * GROUPS, dim), (tok * GROUPS, dim))
    inside = pl.BlockSpec(memory_space=pltpu.VMEM)
    parts = pl.pallas_call(
        functools.partial(kernel, tok, nctx, doc_lengths.shape[0]),
        out_shape=tuple(pltpu.VMEM(shape, bf) for shape in shapes),
        in_specs=[anywhere] * 4 + [pl.BlockSpec(memory_space=pltpu.SMEM)],
        out_specs=(inside,) * 3,
        scratch_shapes=[
            pltpu.VMEM((tok, heads, dim), bf),
            pltpu.VMEM((tok, heads, dim), bf),
            pltpu.VMEM((tok * GROUPS, dim), bf),
            pltpu.VMEM((tok * GROUPS, dim), bf),
            pltpu.VMEM((2, tok * GROUPS, dim), f32),
            pltpu.VMEM((GROUPS, 2, (SLOTS + 1) * tok, dim), bf),
            pltpu.VMEM((GROUPS, qrows, dim), bf),
            pltpu.VMEM((GROUPS, dim, qrows), bf),
            pltpu.VMEM((GROUPS, qrows, dim), bf),
            pltpu.VMEM((GROUPS, dim, qrows), bf),
            pltpu.VMEM((1, qrows), jnp.int32),
            pltpu.VMEM((1, qrows), jnp.int32),
            pltpu.VMEM((GROUPS, SLOTS, qrows), f32),
            pltpu.VMEM((GROUPS, qrows), f32),
            pltpu.VMEM((GROUPS, qrows), f32),
            pltpu.VMEM((GROUPS, SLOTS * tok, qrows), f32),
            pltpu.VMEM((GROUPS, SLOTS * tok, qrows), f32),
            pltpu.VMEM((GROUPS, SLOTS * tok, qrows), bf),
            pltpu.VMEM((SLOTS + 1, 4, tok, dim), f32),
            pltpu.VMEM((SLOTS, 4, tok, dim), bf),
            pltpu.VMEM((SLOTS, 4, tok, dim), bf),
            pltpu.VMEM((GROUPS, qrows, dim), f32),
            pltpu.SemaphoreType.DMA((4,)),
            pltpu.SemaphoreType.DMA((SLOTS, 4)),
            pltpu.SemaphoreType.DMA((SLOTS, 4)),
            pltpu.SemaphoreType.DMA((SLOTS, 4)),
            pltpu.SemaphoreType.DMA((SLOTS, 4)),
        ],
        compiler_params=pltpu.CompilerParams(
            collective_id=0, has_side_effects=True, vmem_limit_bytes=64_500_000
        ),
    )(
        queries,
        key_vectors.reshape(tok * GROUPS, dim),
        value_matrix.reshape(tok * GROUPS, dim),
        grad_out,
        doc_lengths,
    )
    dq, dk, dv = pl.pallas_call(
        writer,
        out_shape=tuple(jax.ShapeDtypeStruct(shape, bf) for shape in shapes),
        in_specs=[anywhere] * 3,
        out_specs=(anywhere,) * 3,
        scratch_shapes=[pltpu.SemaphoreType.DMA((3,))],
        compiler_params=pltpu.CompilerParams(vmem_limit_bytes=1_000_000),
    )(*[pltpu.with_memory_space_constraint(part, pltpu.VMEM) for part in parts])
    return dq, dk.reshape(tok, GROUPS, dim), dv.reshape(tok, GROUPS, dim)


def solution(mesh):
    spec = P("ctx", "tp", None)
    return jax.shard_map(
        functools.partial(local, mesh.shape["ctx"]),
        mesh=mesh,
        in_specs=(spec, spec, spec, spec, P()),
        out_specs=(spec, spec, spec),
        check_vma=False,
    )
```
